8 devices in a mesh: batch: 2 (over z, y), col: 4 (over x, core).
Axes of the slice: x: 2, y: 2, z: 1, core: 2. Of those that a mesh axis runs over, the one named last changes fastest.
Arguments:
- lower: bfloat16 [10240, 5120], P('batch', 'col'), parts along dimension 0
- rhs: bfloat16 [10240, 32768], P('batch', 'col'), parts along dimension 0
Outputs:
- output: bfloat16 [10240, 32768], P('batch', 'col'), parts along dimension 0
There are 2 independent parts. The reference program is written for one: setup_inputs(seed, part) draws one part's arguments, and reference() takes and returns one part's arrays. A program takes and returns all parts, laid end to end along the dimension named above; each array names one.
All inputs are finite; a program needn't handle non-finite values.
Results may differ from the reference program's by a relative error of at most 0.001.
Values are sent between devices in bfloat16 or wider.
A program may use at most 1 GiB of HBM per device.

```python
import jax
import jax.numpy as jnp
from jax import lax

N = 5120
BLOCK_SIZE = 256
GROUP = 4
COLS_DEV = 8192

PER_DEV = N // (BLOCK_SIZE * GROUP)
COLUMNS = COLS_DEV * GROUP


def setup_inputs(seed: int = 0, part: int = 0) -> dict:
    base_key = jax.random.fold_in(jax.random.key(seed), part)
    key_lower, key_rhs = jax.random.split(base_key)
    entries = jax.random.normal(key_lower, (N, N), jnp.float32)
    natural = jnp.tril(entries) * (N ** -0.5)
    stored = natural.reshape(N, PER_DEV, GROUP, BLOCK_SIZE).transpose(0, 2, 1, 3).reshape(N, N)
    rhs = jax.random.normal(key_rhs, (N, COLUMNS), jnp.float32)
    return {"lower": stored.astype(jnp.bfloat16), "rhs": rhs.astype(jnp.bfloat16)}


def reference(lower, rhs):
    natural = lower.reshape(N, GROUP, PER_DEV, BLOCK_SIZE).transpose(0, 2, 1, 3).reshape(N, N)
    col_groups = rhs.reshape(N, GROUP, COLS_DEV).transpose(1, 0, 2)

    def one_group(rhs_cols):
        return jnp.dot(natural, rhs_cols, preferred_element_type=jnp.float32).astype(jnp.bfloat16)

    results = lax.map(one_group, col_groups)
    return results.transpose(1, 0, 2).reshape(N, COLUMNS)
```

```python
import functools

import jax
import jax.numpy as jnp
from jax import lax
from jax.experimental import pallas as pl
from jax.experimental.pallas import tpu as pltpu
from jax.sharding import PartitionSpec as P

BF = jnp.bfloat16
F32 = jnp.float32
BLK = 256
SUP = 4 * BLK
TN = 512
NSUP = 5
NT = 16
NT2 = 8
ROWS = (0, 1, 2, 3)

CHUNKS = [(s, t) for s in (4, 3, 2, 1, 0) for t in range(s + 1)]
CHUNK_ID = {st: i for i, st in enumerate(CHUNKS)}
LG_BASE = {0: 0, 1: 4, 2: 12}


def diag_passes(base):
    return [(base + 1, (1, 2, 3)), (base + 2, (2, 3)), (base + 3, (3,))]


def run_tiles(accs, subs, lhs_of, rhs_of, emit, top, n_tiles):
    flat = [(s, k, rows) for s, passes in enumerate(subs) for k, rows in passes]

    def push(k, j):
        for m in range(2):
            pltpu.matmul_push_rhs(rhs_of(k, m, j), staging_register=0, mxu_index=m)

    def acc_pass(s, k, rows):
        for i, r in enumerate(rows):
            lhs = lhs_of(s, k, r)
            for m in range(2):
                pltpu.matmul_acc_lhs(accs[m][r], lhs, load_staged_rhs=0 if i == 0 else None)

    def pops(s, j):
        for r in ROWS:
            for m in range(2):
                emit(s, j, r, m, pltpu.matmul_pop(accs[m][r]))

    def body(j, carry):
        top(j)
        acc_pass(*flat[-1])
        push(flat[0][1], j + 1)
        pops(flat[-1][0], j)
        for i, (s, k, rows) in enumerate(flat[:-1]):
            acc_pass(s, k, rows)
            push(flat[i + 1][1], j + 1)
            if flat[i + 1][0] != s:
                pops(s, j + 1)
        return carry

    lax.fori_loop(-1, n_tiles - 1, body, 0)
    top(n_tiles - 1)
    acc_pass(*flat[-1])
    pops(flat[-1][0], n_tiles - 1)


def when(cond, fn):
    if isinstance(cond, bool):
        if cond:
            fn()
    else:
        pl.when(cond)(fn)


def cols(j):
    return pl.ds(j * TN, TN) if isinstance(j, int) else pl.ds(pl.multiple_of(j * TN, TN), TN)


def gather_kernel(l_ref, b_ref, lg_ref, x1_ref, x2_ref, pf_ref, la, lb, lc, bbuf, pbuf, obuf, own_sem, dsend, drecv, xsend, xrecv,
                  fsend, frecv, bsem, psem, osem, gsem):
    me = lax.axis_index("col")
    core = lax.rem(me, 2)
    chip = me // 2
    sib = me + 1 - 2 * core
    oth = lax.rem(me + 2, 4)
    sib_oth = lax.rem(sib + 2, 4)
    strips = {4: la, 3: lb, 2: lc}

    def own_src(s, t):
        return l_ref.at[pl.ds(SUP * s, SUP), pl.ds(BLK * t, BLK)]

    def place(s, t, dev, far):
        if s not in strips:
            return lg_ref.at[LG_BASE[s] + 4 * t + dev]
        if t == s:
            slot = 4 * s + dev
        else:
            slot = (2 * s if far else 0) + 2 * t + lax.rem(dev, 2)
        return strips[s].at[:, pl.ds(pl.multiple_of(slot * BLK, BLK), BLK)]

    def own_copy(s, t):
        return pltpu.make_async_copy(own_src(s, t), place(s, t, me, False), own_sem.at[CHUNK_ID[s, t]])

    def remote(src, dst, send, recv, dev):
        return pltpu.make_async_remote_copy(src_ref=src, dst_ref=dst, send_sem=send, recv_sem=recv, device_id={"col": dev},
                                            device_id_type=pl.DeviceIdType.MESH)

    def to_sib(s, t):
        i = CHUNK_ID[s, t]
        return remote(own_src(s, t), place(s, t, me, False), dsend.at[i], drecv.at[i], sib)

    def to_oth(s, t):
        i = CHUNK_ID[s, t]
        return remote(own_src(s, t), place(s, t, me, True), xsend.at[i], xrecv.at[i], oth)

    def forward(s, t):
        i = CHUNK_ID[s, t]
        here = place(s, t, oth, True)
        return remote(here, here, fsend.at[i], frecv.at[i], sib)

    def from_sib(s, t):
        i = CHUNK_ID[s, t]
        here = place(s, t, sib, False)
        return remote(here, here, dsend.at[i], drecv.at[i], sib)

    def from_oth(s, t):
        i = CHUNK_ID[s, t]
        here = place(s, t, oth, True)
        return remote(here, here, xsend.at[i], xrecv.at[i], oth)

    def from_fwd(s, t):
        i = CHUNK_ID[s, t]
        here = place(s, t, sib_oth, True)
        return remote(here, here, fsend.at[i], frecv.at[i], sib)

    def pass_on(s, t):
        from_oth(s, t).wait_recv()
        forward(s, t).start()

    jobs = [(4, "part", NT), (3, "part", NT), (4, "rest", NT), (3, "rest", NT), (2, "all", NT2)]
    passes = {"part": lambda s: 2 * s * 512, "rest": lambda s: 2 * s * 512 + 1280, "all": lambda s: 4 * s * 512 + 1280}
    events = [dict() for _ in jobs]
    clock, todo = 6.0, list(enumerate(CHUNKS))
    for q, (s, kind, n) in enumerate(jobs):
        for j in range(n):
            if todo and clock > 5.0 + 11.3 * (todo[0][0] + 1) + 1.5:
                events[q][j] = todo.pop(0)[1]
            clock += passes[kind](s) / 1850.0
    left = [st for _, st in todo]

    def b_copies(q, j, slot):
        s, kind, _ = jobs[q]
        dst = bbuf.at[slot]
        if kind == "part":
            return [pltpu.make_async_copy(b_ref.at[0:s, chip, :, cols(j)], dst.at[0:s], bsem.at[slot, 0])]
        far = pltpu.make_async_copy(b_ref.at[0:s, 1 - chip, :, cols(j)], dst.at[0:s], bsem.at[slot, 0])
        if kind == "rest":
            return [far, pltpu.make_async_copy(b_ref.at[s, :, :, cols(j)], dst.at[pl.ds(s, 2)], bsem.at[slot, 1])]
        return [
            pltpu.make_async_copy(b_ref.at[0:s, chip, :, cols(j)], dst.at[0:s], bsem.at[slot, 0]),
            pltpu.make_async_copy(b_ref.at[0:s, 1 - chip, :, cols(j)], dst.at[pl.ds(s, s)], bsem.at[slot, 2]),
            pltpu.make_async_copy(b_ref.at[s, :, :, cols(j)], dst.at[pl.ds(2 * s, 2)], bsem.at[slot, 1]),
        ]

    def run_job(q):
        s, kind, n = jobs[q]
        lbuf = strips[s]
        nxt = q + 1 if q + 1 < len(jobs) else None

        def start_b(qq, j, slot):
            for c in b_copies(qq, j, slot):
                c.start()

        def out_copy(j):
            slot = j & 1
            if kind == "part":
                return pltpu.make_async_copy(pbuf.at[slot], pf_ref.at[s - 3, :, cols(j)], osem.at[slot])
            if kind == "rest":
                return pltpu.make_async_copy(obuf.at[slot], x1_ref.at[pl.ds(SUP * (s - 3), SUP), cols(j)], osem.at[slot])
            return pltpu.make_async_copy(obuf.at[slot], x2_ref.at[:, cols(j)], osem.at[slot])

        def part_copy(j):
            slot = j & 1
            return pltpu.make_async_copy(pf_ref.at[s - 3, :, cols(j)], pbuf.at[slot], psem.at[slot])

        def body(j, carry):
            slot = j & 1
            pl.when(j < n - 1)(lambda: start_b(q, j + 1, 1 - slot))
            if nxt is not None:
                pl.when(j == n - 1)(lambda: start_b(nxt, 0, 0))
            if events[q]:
                hit = functools.reduce(jnp.logical_or, [j == jj for jj in events[q]])

                @pl.when(hit)
                def _():
                    for jj, st in events[q].items():
                        pl.when(j == jj)(functools.partial(pass_on, *st))

            pl.when(j >= 1)(lambda: out_copy(j - 1).start())
            pl.when(j >= 2)(lambda: out_copy(j - 2).wait())
            if kind == "rest":
                pl.when(j < n - 1)(lambda: part_copy(j + 1).start())
                part_copy(j).wait()
            for c in b_copies(q, j, slot):
                c.wait()
            base = 0 if kind == "part" else (2 * s if kind == "rest" else 0)
            for r in ROWS:
                rows = slice(r * BLK, (r + 1) * BLK)
                n_k = 2 * s if kind == "part" else (4 * s + r + 1 - base)
                rhs = bbuf[slot, 0:(n_k + 1) // 2].reshape(-1, TN)[0:n_k * BLK]
                v = jnp.dot(lbuf[rows, base * BLK:(base + n_k) * BLK], rhs, preferred_element_type=F32)
                if kind == "part":
                    pbuf[slot, rows, :] = v
                elif kind == "rest":
                    obuf[slot, rows, :] = (v + pbuf[slot, rows, :]).astype(BF)
                else:
                    obuf[slot, rows, :] = v.astype(BF)
            return carry

        if kind == "rest":
            part_copy(0).start()
        lax.fori_loop(0, n, body, 0)
        out_copy(n - 1).start()
        out_copy(n - 2).wait()
        out_copy(n - 1).wait()

    def inner():
        for s in (4, 3, 2):
            for t in range(s + 1):
                own_copy(s, t).start()
        for c in b_copies(0, 0, 0):
            c.start()
        barrier = pltpu.get_barrier_semaphore()
        for dev in (sib, oth):
            pl.semaphore_signal(barrier, inc=1, device_id={"col": dev}, device_id_type=pl.DeviceIdType.MESH)
        pl.semaphore_wait(barrier, 2)
        for t in range(5):
            to_sib(4, t).start()
        for s, t in CHUNKS:
            to_oth(s, t).start()
        for s, t in CHUNKS[5:]:
            to_sib(s, t).start()

        for s, t in CHUNKS[:12]:
            own_copy(s, t).wait()
        for t in range(4):
            from_sib(4, t).wait_recv()
        run_job(0)
        for t in range(3):
            from_sib(3, t).wait_recv()
        run_job(1)
        from_sib(4, 4).wait_recv()
        for t in range(5):
            from_fwd(4, t).wait_recv()
        run_job(2)
        from_sib(3, 3).wait_recv()
        for t in range(4):
            from_fwd(3, t).wait_recv()
        run_job(3)
        for t in range(3):
            from_sib(2, t).wait_recv()
            from_fwd(2, t).wait_recv()
        saves = []
        for k in range(12):
            t, u = k % 4 // 2, k % 2
            kb = k if k >= 8 else 4 * t + 2 * (chip if k < 4 else 1 - chip) + u
            saves.append(pltpu.make_async_copy(lc.at[:, pl.ds(k * BLK, BLK)], lg_ref.at[LG_BASE[2] + kb], gsem.at[k]))
        for c in saves:
            c.start()
        run_job(4)
        for s, t in left:
            pass_on(s, t)
        for c in saves:
            c.wait()
        for s in (1, 0):
            for t in range(s + 1):
                from_sib(s, t).wait_recv()
                from_fwd(s, t).wait_recv()
        for s, t in CHUNKS:
            to_sib(s, t).wait_send()
            to_oth(s, t).wait_send()
            forward(s, t).wait_send()

    inner()


def finish_kernel(l_ref, b_ref, lg_ref, x1_ref, x2_ref, x_ref, lbuf, bbuf, obuf, cbuf, dbuf, lsem, bsem, osem, csem, dsem):
    me = lax.axis_index("col")
    jobs = [(0, NT2, (0, 1)), (NT2, NT - NT2, (0, 1, 2))]

    def l_copies(s):
        base = LG_BASE[s]
        if s == 2:
            return [pltpu.make_async_copy(lg_ref.at[pl.ds(base, 12)], lbuf.at[pl.ds(base, 12)], lsem.at[base])]
        out = []
        for t in range(s + 1):
            for d in range(4):
                at = base + 4 * t + lax.rem(me + d, 4)
                src = l_ref.at[pl.ds(SUP * s, SUP), pl.ds(BLK * t, BLK)] if d == 0 else lg_ref.at[at]
                out.append(pltpu.make_async_copy(src, lbuf.at[at], lsem.at[base + 4 * t + d]))
        return out

    def b_copy(q, j, slot):
        n = 4 * len(jobs[q][2])
        return pltpu.make_async_copy(b_ref.at[0:n, :, cols(jobs[q][0] + j)], bbuf.at[slot, 0:n], bsem.at[slot])

    def run_job(q, accs):
        first, n, sups = jobs[q]
        nxt = q + 1 if q + 1 < len(jobs) else None
        lasts = len(sups) - 1

        def out_copy(u, j):
            slot = j & 1
            return pltpu.make_async_copy(obuf.at[slot, u], x_ref.at[pl.ds(SUP * sups[u], SUP), cols(first + j)], osem.at[slot, u])

        if q == 0:
            rows = SUP // n

            def c_in(j):
                return pltpu.make_async_copy(x2_ref.at[pl.ds(pl.multiple_of(j * rows, rows), rows), :], dbuf.at[j & 1], dsem.at[0, j & 1])

            def c_out(j):
                return pltpu.make_async_copy(
                    dbuf.at[j & 1], x_ref.at[pl.ds(pl.multiple_of(2 * SUP + j * rows, rows), rows), pl.ds(0, NT2 * TN)], dsem.at[1, j & 1])
        else:
            rows = 2 * SUP // n

            def c_in(j):
                return pltpu.make_async_copy(x1_ref.at[pl.ds(pl.multiple_of(j * rows, rows), rows), :], cbuf.at[j & 1], csem.at[0, j & 1])

            def c_out(j):
                return pltpu.make_async_copy(
                    cbuf.at[j & 1], x_ref.at[pl.ds(pl.multiple_of(3 * SUP + j * rows, rows), rows), :], csem.at[1, j & 1])

        def top(j):
            last = isinstance(j, int)
            if not last:
                b_copy(q, j + 1, (j + 1) & 1).wait()
                lo = -1 if q == 0 else 0
                pl.when(jnp.logical_and(j >= lo, j < n - 2))(lambda: b_copy(q, j + 2, j & 1).start())
                if nxt is not None:
                    pl.when(j == n - 2)(lambda: b_copy(nxt, 0, 0).start())
            elif nxt is not None:
                b_copy(nxt, 1, 1).start()
            for u in range(len(sups)):
                if u < lasts:
                    when(True if last else j >= 0, lambda: out_copy(u, j).start())
                    when(True if last else j >= 1, lambda: out_copy(u, j - 1).wait())
                else:
                    when(True if last else j >= 1, lambda: out_copy(u, j - 1).start())
                    when(True if last else j >= 2, lambda: out_copy(u, j - 2).wait())
            if not last:
                pl.when(j >= 1)(lambda: c_out(j - 1).wait())
                c_in(j + 1).start()
            when(True if last else j >= 0, lambda: c_in(j).wait())
            when(True if last else j >= 0, lambda: c_out(j).start())

        def lhs_of(u, k, r):
            return lbuf[LG_BASE[sups[u]] + k, r * BLK:(r + 1) * BLK, :]

        def rhs_of(k, m, j):
            return bbuf[j & 1, k, :, m * BLK:(m + 1) * BLK]

        def emit(u, j, r, m, v):
            obuf[j & 1, u, r * BLK:(r + 1) * BLK, m * BLK:(m + 1) * BLK] = v.astype(BF)

        subs = [diag_passes(4 * s) + [(4 * s, ROWS)] + [(k, ROWS) for k in range(4 * s)] for s in sups]
        run_tiles(accs, subs, lhs_of, rhs_of, emit, top, n)
        out_copy(lasts, n - 1).start()
        c_out(n - 2).wait()
        c_out(n - 1).wait()
        for u in range(len(sups)):
            if u == lasts:
                out_copy(u, n - 2).wait()
            out_copy(u, n - 1).wait()

    def inner(*refs):
        accs = (refs[:4], refs[4:])
        b_copy(0, 0, 0).start()
        for s in (0, 1, 2):
            for c in l_copies(s):
                c.start()
        for s in (0, 1):
            for c in l_copies(s):
                c.wait()
        run_job(0, accs)
        for c in l_copies(2):
            c.wait()
        run_job(1, accs)

    pl.run_scoped(inner, *[pltpu.ACC(m)((BLK, BLK), F32) for m in range(2) for _ in ROWS])


def solution(mesh):
    hbm = pl.BlockSpec(memory_space=pltpu.HBM)
    dma = pltpu.SemaphoreType.DMA

    def local_product(l_cols, b_cols):
        order, width = b_cols.shape
        b4 = b_cols.reshape(NSUP, 2, 2 * BLK, width)
        b3 = b_cols.reshape(4 * NSUP, BLK, width)
        lg, x1, x2, _ = pl.pallas_call(
            gather_kernel,
            out_shape=(
                jax.ShapeDtypeStruct((24, SUP, BLK), BF),
                jax.ShapeDtypeStruct((2 * SUP, width), BF),
                jax.ShapeDtypeStruct((SUP, NT2 * TN), BF),
                jax.ShapeDtypeStruct((2, SUP, width), F32),
            ),
            in_specs=[hbm] * 2,
            out_specs=(hbm,) * 4,
            scratch_shapes=[
                pltpu.VMEM((SUP, 20 * BLK), BF),
                pltpu.VMEM((SUP, 16 * BLK), BF),
                pltpu.VMEM((SUP, 12 * BLK), BF),
                pltpu.VMEM((2, 6, 2 * BLK, TN), BF),
                pltpu.VMEM((2, SUP, TN), F32),
                pltpu.VMEM((2, SUP, TN), BF),
            ] + [dma((15,))] * 7 + [dma((2, 3)), dma((2,)), dma((2,)), dma((12,))],
            compiler_params=pltpu.CompilerParams(vmem_limit_bytes=62 * 1024 * 1024, collective_id=0, has_side_effects=True),
        )(l_cols, b4)
        return pl.pallas_call(
            finish_kernel,
            out_shape=jax.ShapeDtypeStruct((order, width), BF),
            in_specs=[hbm] * 5,
            out_specs=hbm,
            scratch_shapes=[
                pltpu.VMEM((24, SUP, BLK), BF),
                pltpu.VMEM((2, 12, BLK, TN), BF),
                pltpu.VMEM((2, 3, SUP, TN), BF),
                pltpu.VMEM((2, 2 * SUP // (NT - NT2), width), BF),
                pltpu.VMEM((2, SUP // NT2, NT2 * TN), BF),
            ] + [dma((24,)), dma((2,)), dma((2, 3)), dma((2, 2)), dma((2, 2))],
            compiler_params=pltpu.CompilerParams(vmem_limit_bytes=62 * 1024 * 1024),
        )(l_cols, b3, lg, x1, x2)

    return jax.shard_map(local_product, mesh=mesh, in_specs=(P("batch", "col"), P("batch", "col")), out_specs=P("batch", "col"), check_vma=False)
```

```python
import functools

import jax
import jax.numpy as jnp
from jax import lax
from jax.experimental import pallas as pl
from jax.experimental.pallas import tpu as pltpu
from jax.sharding import PartitionSpec as P

BF = jnp.bfloat16
F32 = jnp.float32
BLK = 256
SUP = 4 * BLK
TN = 512
NSUP = 5
WIDE = 1024
DN = 512
NT = 8
NT2 = 2
N0 = NT2 * WIDE // TN
N1 = (NT - NT2) * WIDE // TN
ROWS = (0, 1, 2, 3)

CHUNKS = [(s, t) for s in (4, 3, 2, 1, 0) for t in range(s + 1)]
CHUNK_ID = {st: i for i, st in enumerate(CHUNKS)}
LG_BASE = {0: 0, 1: 4, 2: 12}


def diag_passes(base):
    return [(base + 1, (1, 2, 3)), (base + 2, (2, 3)), (base + 3, (3,))]


def run_tiles(accs, subs, lhs_of, rhs_of, emit, top, n_tiles):
    flat = [(s, k, rows) for s, passes in enumerate(subs) for k, rows in passes]

    def push(k, j):
        for m in range(2):
            pltpu.matmul_push_rhs(rhs_of(k, m, j), staging_register=0, mxu_index=m)

    def acc_pass(s, k, rows):
        for i, r in enumerate(rows):
            lhs = lhs_of(s, k, r)
            for m in range(2):
                pltpu.matmul_acc_lhs(accs[m][r], lhs, load_staged_rhs=0 if i == 0 else None)

    def pops(s, j):
        for r in ROWS:
            for m in range(2):
                emit(s, j, r, m, pltpu.matmul_pop(accs[m][r]))

    def body(j, carry):
        top(j)
        acc_pass(*flat[-1])
        push(flat[0][1], j + 1)
        pops(flat[-1][0], j)
        for i, (s, k, rows) in enumerate(flat[:-1]):
            acc_pass(s, k, rows)
            push(flat[i + 1][1], j + 1)
            if flat[i + 1][0] != s:
                pops(s, j + 1)
        return carry

    lax.fori_loop(-1, n_tiles - 1, body, 0)
    top(n_tiles - 1)
    acc_pass(*flat[-1])
    pops(flat[-1][0], n_tiles - 1)


def when(cond, fn):
    if isinstance(cond, bool):
        if cond:
            fn()
    else:
        pl.when(cond)(fn)


def cols(j):
    return pl.ds(j * TN, TN) if isinstance(j, int) else pl.ds(pl.multiple_of(j * TN, TN), TN)


def wide(j):
    return pl.ds(pl.multiple_of(j * WIDE, WIDE), WIDE)


def gather_kernel(l_ref, b_ref, lg_ref, x1_ref, x2_ref, pf_ref, la, lb, lc, bbuf, pbuf, pin, obuf, own_sem, dsend, drecv, xsend, xrecv,
                  fsend, frecv, bsem, psem, osem, gsem):
    me = lax.axis_index("col")
    core = lax.rem(me, 2)
    chip = me // 2
    sib = me + 1 - 2 * core
    oth = lax.rem(me + 2, 4)
    sib_oth = lax.rem(sib + 2, 4)
    strips = {4: la, 3: lb, 2: lc}

    def own_src(s, t):
        return l_ref.at[pl.ds(SUP * s, SUP), pl.ds(BLK * t, BLK)]

    def place(s, t, dev, far):
        if s not in strips:
            return lg_ref.at[LG_BASE[s] + 4 * t + dev]
        if t == s:
            slot = 4 * s + dev
        else:
            slot = (2 * s if far else 0) + 2 * t + lax.rem(dev, 2)
        return strips[s].at[:, pl.ds(pl.multiple_of(slot * BLK, BLK), BLK)]

    def own_copy(s, t):
        return pltpu.make_async_copy(own_src(s, t), place(s, t, me, False), own_sem.at[CHUNK_ID[s, t]])

    def remote(src, dst, send, recv, dev):
        return pltpu.make_async_remote_copy(src_ref=src, dst_ref=dst, send_sem=send, recv_sem=recv, device_id={"col": dev},
                                            device_id_type=pl.DeviceIdType.MESH)

    def to_sib(s, t):
        i = CHUNK_ID[s, t]
        return remote(own_src(s, t), place(s, t, me, False), dsend.at[i], drecv.at[i], sib)

    def to_oth(s, t):
        i = CHUNK_ID[s, t]
        return remote(own_src(s, t), place(s, t, me, True), xsend.at[i], xrecv.at[i], oth)

    def forward(s, t):
        i = CHUNK_ID[s, t]
        here = place(s, t, oth, True)
        return remote(here, here, fsend.at[i], frecv.at[i], sib)

    def from_sib(s, t):
        i = CHUNK_ID[s, t]
        here = place(s, t, sib, False)
        return remote(here, here, dsend.at[i], drecv.at[i], sib)

    def from_oth(s, t):
        i = CHUNK_ID[s, t]
        here = place(s, t, oth, True)
        return remote(here, here, xsend.at[i], xrecv.at[i], oth)

    def from_fwd(s, t):
        i = CHUNK_ID[s, t]
        here = place(s, t, sib_oth, True)
        return remote(here, here, fsend.at[i], frecv.at[i], sib)

    def pass_on(s, t):
        from_oth(s, t).wait_recv()
        forward(s, t).start()

    jobs = [((4, 3), "part", NT), ((4,), "rest", NT), ((3,), "rest", NT), ((2,), "all", NT2)]
    cycles = {"part": lambda s: 2 * s * 512, "rest": lambda s: 2 * s * 512 + 1280, "all": lambda s: 4 * s * 512 + 1280}
    events, forced = [[] for _ in jobs], [[] for _ in jobs]
    clock, todo = 5.0, list(enumerate(CHUNKS))
    for q, (sups, kind, n) in enumerate(jobs):
        while kind != "part" and todo and todo[0][1][0] >= sups[0]:
            i, st = todo.pop(0)
            clock = max(clock, 5.0 + 11.3 * (i + 1))
            forced[q].append(st)
        for j in range(n):
            while todo and clock > 5.0 + 11.3 * (todo[0][0] + 1) + 1.0:
                events[q].append((j, todo.pop(0)[1]))
            clock += 2 * sum(map(cycles[kind], sups)) / 1850.0
    left = [st for _, st in todo]

    def b_copies(q, j, slot):
        s, kind = jobs[q][0][0], jobs[q][1]
        dst = bbuf.at[slot]
        if kind == "part":
            return [pltpu.make_async_copy(b_ref.at[0:s, chip, :, wide(j)], dst.at[0:s], bsem.at[slot, 0])]
        far = pltpu.make_async_copy(b_ref.at[0:s, 1 - chip, :, wide(j)], dst.at[0:s], bsem.at[slot, 0])
        if kind == "rest":
            return [far, pltpu.make_async_copy(b_ref.at[s, :, :, wide(j)], dst.at[pl.ds(s, 2)], bsem.at[slot, 1])]
        return [
            pltpu.make_async_copy(b_ref.at[0:s, chip, :, wide(j)], dst.at[0:s], bsem.at[slot, 0]),
            pltpu.make_async_copy(b_ref.at[0:s, 1 - chip, :, wide(j)], dst.at[pl.ds(s, s)], bsem.at[slot, 2]),
            pltpu.make_async_copy(b_ref.at[s, :, :, wide(j)], dst.at[pl.ds(2 * s, 2)], bsem.at[slot, 1]),
        ]

    def run_job(q):
        sups, kind, n = jobs[q]
        nxt = q + 1 if q + 1 < len(jobs) else None

        def start_b(qq, j, slot):
            for c in b_copies(qq, j, slot):
                c.start()

        def x_copy(qq, j):
            (ss, *_), kk, _ = jobs[qq]
            dst = x1_ref.at[pl.ds(SUP * (ss - 3), SUP), wide(j)] if kk == "rest" else x2_ref.at[:, wide(j)]
            return pltpu.make_async_copy(obuf.at[j & 1], dst, osem.at[j & 1])

        def pf_out(i, j):
            return pltpu.make_async_copy(pbuf.at[i], pf_ref.at[1 - i, :, wide(j)], gsem.at[i])

        def part_copy(qq, j):
            return pltpu.make_async_copy(pf_ref.at[jobs[qq][0][0] - 3, :, wide(j)], pin.at[j & 1], psem.at[j & 1])

        def body(j, carry):
            slot = j & 1

            @pl.when(j < n - 1)
            def _():
                start_b(q, j + 1, 1 - slot)
                if kind == "rest":
                    part_copy(q, j + 1).start()

            if nxt is not None:

                @pl.when(j == n - 1)
                def _():
                    start_b(nxt, 0, 0)
                    if jobs[nxt][1] == "rest":
                        part_copy(nxt, 0).start()

            if events[q]:
                hit = functools.reduce(jnp.logical_or, [j == jj for jj, _ in events[q]])

                @pl.when(hit)
                def _():
                    for jj, st in events[q]:
                        pl.when(j == jj)(functools.partial(pass_on, *st))

            if kind == "part":
                pl.when(j >= 1)(lambda: pf_out(1, j - 1).start())
            else:

                @pl.when(j == 0)
                def _():
                    if q == 1:
                        pf_out(1, NT - 1).start()
                        pf_out(0, NT - 1).wait()
                    else:
                        x_copy(q - 1, jobs[q - 1][2] - 1).start()
                        x_copy(q - 1, jobs[q - 1][2] - 2).wait()

                @pl.when(j == 1)
                def _():
                    x_copy(q, 0).start()
                    if q == 1:
                        pf_out(1, NT - 1).wait()
                    else:
                        x_copy(q - 1, jobs[q - 1][2] - 1).wait()

                @pl.when(j >= 2)
                def _():
                    x_copy(q, j - 1).start()
                    x_copy(q, j - 2).wait()

            if kind == "rest":
                part_copy(q, j).wait()
            for c in b_copies(q, j, slot):
                c.wait()
            for i, s in enumerate(sups):
                if kind == "part":
                    pl.when(j >= 1)(lambda: pf_out(i, j - 1).wait())
                    if i == 1:

                        @pl.when(j == 0)
                        def _():
                            for t in range(3):
                                own_copy(3, t).wait()
                                from_sib(3, t).wait_recv()

                base = 2 * s if kind == "rest" else 0
                for r in ROWS:
                    rows = slice(r * BLK, (r + 1) * BLK)
                    n_k = 2 * s if kind == "part" else 4 * s + r + 1 - base
                    for h in range(WIDE // DN):
                        half = slice(h * DN, (h + 1) * DN)
                        rhs = bbuf[slot, 0:(n_k + 1) // 2, :, half].reshape(-1, DN)[0:n_k * BLK]
                        v = jnp.dot(strips[s][rows, base * BLK:(base + n_k) * BLK], rhs, preferred_element_type=F32)
                        if kind == "part":
                            pbuf[i, rows, half] = v
                        elif kind == "rest":
                            obuf[slot, rows, half] = (v + pin[slot, rows, half]).astype(BF)
                        else:
                            obuf[slot, rows, half] = v.astype(BF)
                    if kind == "part" and (i, r) == (1, 0):
                        pf_out(0, j).start()
            return carry

        lax.fori_loop(0, n, body, 0)
        if nxt is None:
            x_copy(q, n - 1).start()
            x_copy(q, n - 2).wait()
            x_copy(q, n - 1).wait()

    def inner():
        for c in b_copies(0, 0, 0):
            c.start()
        early = [(4, t) for t in range(4)] + [(3, t) for t in range(3)]
        for st in early:
            own_copy(*st).start()
        barrier = pltpu.get_barrier_semaphore()
        for dev in (sib, oth):
            pl.semaphore_signal(barrier, inc=1, device_id={"col": dev}, device_id_type=pl.DeviceIdType.MESH)
        pl.semaphore_wait(barrier, 2)
        for st in early:
            to_sib(*st).start()
        for st in CHUNKS:
            to_oth(*st).start()
        for st in CHUNKS:
            if st not in early:
                to_sib(*st).start()
                if st[0] >= 2:
                    own_copy(*st).start()

        for t in range(4):
            own_copy(4, t).wait()
            from_sib(4, t).wait_recv()
        run_job(0)
        for q, s in ((1, 4), (2, 3), (3, 2)):
            for st in forced[q]:
                pass_on(*st)
            for t in range(s + 1):
                if t == s or s == 2:
                    own_copy(s, t).wait()
                    from_sib(s, t).wait_recv()
                from_fwd(s, t).wait_recv()
            if s > 2:
                run_job(q)
        saves = []
        for k in range(12):
            t, u = k % 4 // 2, k % 2
            kb = k if k >= 8 else 4 * t + 2 * (chip if k < 4 else 1 - chip) + u
            saves.append(pltpu.make_async_copy(lc.at[:, pl.ds(k * BLK, BLK)], lg_ref.at[LG_BASE[2] + kb], gsem.at[2 + k]))
        for c in saves:
            c.start()
        run_job(3)
        for s, t in left:
            pass_on(s, t)
        for c in saves:
            c.wait()
        for s in (1, 0):
            for t in range(s + 1):
                from_sib(s, t).wait_recv()
                from_fwd(s, t).wait_recv()
        for s, t in CHUNKS:
            to_sib(s, t).wait_send()
            to_oth(s, t).wait_send()
            forward(s, t).wait_send()

    inner()


def finish_kernel(l_ref, b_ref, lg_ref, x1_ref, x2_ref, x_ref, lbuf, bbuf, obuf, cbuf, dbuf, lsem, bsem, osem, csem, dsem):
    me = lax.axis_index("col")
    jobs = [(0, N0, (0, 1)), (N0, N1, (0, 1, 2))]

    def l_copies(s):
        base = LG_BASE[s]
        if s == 2:
            return [pltpu.make_async_copy(lg_ref.at[pl.ds(base, 12)], lbuf.at[pl.ds(base, 12)], lsem.at[base])]
        out = []
        for t in range(s + 1):
            for d in range(4):
                at = base + 4 * t + lax.rem(me + d, 4)
                src = l_ref.at[pl.ds(SUP * s, SUP), pl.ds(BLK * t, BLK)] if d == 0 else lg_ref.at[at]
                out.append(pltpu.make_async_copy(src, lbuf.at[at], lsem.at[base + 4 * t + d]))
        return out

    def b_copy(q, j, slot):
        n = 4 * len(jobs[q][2])
        return pltpu.make_async_copy(b_ref.at[0:n, :, cols(jobs[q][0] + j)], bbuf.at[slot, 0:n], bsem.at[slot])

    def run_job(q, accs):
        first, n, sups = jobs[q]
        nxt = q + 1 if q + 1 < len(jobs) else None
        lasts = len(sups) - 1

        def out_copy(u, j):
            slot = j & 1
            return pltpu.make_async_copy(obuf.at[slot, u], x_ref.at[pl.ds(SUP * sups[u], SUP), cols(first + j)], osem.at[slot, u])

        if q == 0:
            chunks = n
            rows = SUP // chunks

            def c_in(j):
                return pltpu.make_async_copy(x2_ref.at[pl.ds(pl.multiple_of(j * rows, rows), rows), :], dbuf.at[j & 1], dsem.at[0, j & 1])

            def c_out(j):
                return pltpu.make_async_copy(
                    dbuf.at[j & 1], x_ref.at[pl.ds(pl.multiple_of(2 * SUP + j * rows, rows), rows), pl.ds(0, N0 * TN)], dsem.at[1, j & 1])
        else:
            chunks = 8
            rows = 2 * SUP // chunks

            def c_in(j):
                return pltpu.make_async_copy(x1_ref.at[pl.ds(pl.multiple_of(j * rows, rows), rows), :], cbuf.at[j & 1], csem.at[0, j & 1])

            def c_out(j):
                return pltpu.make_async_copy(
                    cbuf.at[j & 1], x_ref.at[pl.ds(pl.multiple_of(3 * SUP + j * rows, rows), rows), :], csem.at[1, j & 1])

        def top(j):
            last = isinstance(j, int)
            if not last:
                b_copy(q, j + 1, (j + 1) & 1).wait()
                lo = -1 if q == 0 else 0
                pl.when(jnp.logical_and(j >= lo, j < n - 2))(lambda: b_copy(q, j + 2, j & 1).start())
                if nxt is not None:
                    pl.when(j == n - 2)(lambda: b_copy(nxt, 0, 0).start())
            elif nxt is not None:
                b_copy(nxt, 1, 1).start()
            for u in range(len(sups)):
                if u < lasts:
                    when(True if last else j >= 0, lambda: out_copy(u, j).start())
                    when(True if last else j >= 1, lambda: out_copy(u, j - 1).wait())
                else:
                    when(True if last else j >= 1, lambda: out_copy(u, j - 1).start())
                    when(True if last else j >= 2, lambda: out_copy(u, j - 2).wait())
            if not last:
                pl.when(jnp.logical_and(j >= 1, j <= chunks))(lambda: c_out(j - 1).wait())
                pl.when(j + 1 < chunks)(lambda: c_in(j + 1).start())
            if not last or j < chunks:

                def move():
                    c_in(j).wait()
                    c_out(j).start()

                when(True if last else jnp.logical_and(j >= 0, j < chunks), move)

        def lhs_of(u, k, r):
            return lbuf[LG_BASE[sups[u]] + k, r * BLK:(r + 1) * BLK, :]

        def rhs_of(k, m, j):
            return bbuf[j & 1, k, :, m * BLK:(m + 1) * BLK]

        def emit(u, j, r, m, v):
            obuf[j & 1, u, r * BLK:(r + 1) * BLK, m * BLK:(m + 1) * BLK] = v.astype(BF)

        subs = [diag_passes(4 * s) + [(4 * s, ROWS)] + [(k, ROWS) for k in range(4 * s)] for s in sups]
        run_tiles(accs, subs, lhs_of, rhs_of, emit, top, n)
        out_copy(lasts, n - 1).start()
        if chunks == n:
            c_out(n - 2).wait()
            c_out(n - 1).wait()
        for u in range(len(sups)):
            if u == lasts:
                out_copy(u, n - 2).wait()
            out_copy(u, n - 1).wait()

    def inner(*refs):
        accs = (refs[:4], refs[4:])
        b_copy(0, 0, 0).start()
        for s in (0, 1, 2):
            for c in l_copies(s):
                c.start()
        for s in (0, 1):
            for c in l_copies(s):
                c.wait()
        run_job(0, accs)
        for c in l_copies(2):
            c.wait()
        run_job(1, accs)

    pl.run_scoped(inner, *[pltpu.ACC(m)((BLK, BLK), F32) for m in range(2) for _ in ROWS])


def solution(mesh):
    hbm = pl.BlockSpec(memory_space=pltpu.HBM)
    dma = pltpu.SemaphoreType.DMA

    def local_product(l_cols, b_cols):
        order, width = b_cols.shape
        b4 = b_cols.reshape(NSUP, 2, 2 * BLK, width)
        b3 = b_cols.reshape(4 * NSUP, BLK, width)
        lg, x1, x2, _ = pl.pallas_call(
            gather_kernel,
            out_shape=(
                jax.ShapeDtypeStruct((24, SUP, BLK), BF),
                jax.ShapeDtypeStruct((2 * SUP, width), BF),
                jax.ShapeDtypeStruct((SUP, N0 * TN), BF),
                jax.ShapeDtypeStruct((2, SUP, width), F32),
            ),
            in_specs=[hbm] * 2,
            out_specs=(hbm,) * 4,
            scratch_shapes=[
                pltpu.VMEM((SUP, 20 * BLK), BF),
                pltpu.VMEM((SUP, 16 * BLK), BF),
                pltpu.VMEM((SUP, 12 * BLK), BF),
                pltpu.VMEM((2, 6, 2 * BLK, WIDE), BF),
                pltpu.VMEM((2, SUP, WIDE), F32),
                pltpu.VMEM((2, SUP, WIDE), F32),
                pltpu.VMEM((2, SUP, WIDE), BF),
            ] + [dma((15,))] * 7 + [dma((2, 3)), dma((2,)), dma((2,)), dma((14,))],
            compiler_params=pltpu.CompilerParams(vmem_limit_bytes=62 * 1024 * 1024, collective_id=0, has_side_effects=True),
        )(l_cols, b4)
        return pl.pallas_call(
            finish_kernel,
            out_shape=jax.ShapeDtypeStruct((order, width), BF),
            in_specs=[hbm] * 5,
            out_specs=hbm,
            scratch_shapes=[
                pltpu.VMEM((24, SUP, BLK), BF),
                pltpu.VMEM((2, 12, BLK, TN), BF),
                pltpu.VMEM((2, 3, SUP, TN), BF),
                pltpu.VMEM((2, 2 * SUP // 8, width), BF),
                pltpu.VMEM((2, SUP // N0, N0 * TN), BF),
            ] + [dma((24,)), dma((2,)), dma((2, 3)), dma((2, 2)), dma((2, 2))],
            compiler_params=pltpu.CompilerParams(vmem_limit_bytes=62 * 1024 * 1024),
        )(l_cols, b3, lg, x1, x2)

    return jax.shard_map(local_product, mesh=mesh, in_specs=(P("batch", "col"), P("batch", "col")), out_specs=P("batch", "col"), check_vma=False)
```

```python
import functools

import jax
import jax.numpy as jnp
from jax import lax
from jax.experimental import pallas as pl
from jax.experimental.pallas import tpu as pltpu
from jax.sharding import PartitionSpec as P

BF = jnp.bfloat16
F32 = jnp.float32
BLK = 256
SUP = 4 * BLK
TN = 512
NSUP = 5
WIDE = 1024
DN = 512
NT = 8
NT2 = 2
N0 = NT2 * WIDE // TN
N1 = (NT - NT2) * WIDE // TN
COPY = -(-2 * SUP // N1 // 16) * 16
ROWS = (0, 1, 2, 3)

CHUNKS = [(s, t) for s in (4, 3, 2, 1, 0) for t in range(s + 1)]
CHUNK_ID = {st: i for i, st in enumerate(CHUNKS)}
LG_BASE = {0: 0, 1: 4, 2: 12}


def diag_passes(base):
    return [(base + 1, (1, 2, 3)), (base + 2, (2, 3)), (base + 3, (3,))]


def run_tiles(accs, subs, lhs_of, rhs_of, emit, top, n_tiles):
    flat = [(s, k, rows) for s, passes in enumerate(subs) for k, rows in passes]

    def push(k, j):
        for m in range(2):
            pltpu.matmul_push_rhs(rhs_of(k, m, j), staging_register=0, mxu_index=m)

    def acc_pass(s, k, rows):
        for i, r in enumerate(rows):
            lhs = lhs_of(s, k, r)
            for m in range(2):
                pltpu.matmul_acc_lhs(accs[m][r], lhs, load_staged_rhs=0 if i == 0 else None)

    def pops(s, j):
        for r in ROWS:
            for m in range(2):
                emit(s, j, r, m, pltpu.matmul_pop(accs[m][r]))

    def body(j, carry):
        top(j)
        acc_pass(*flat[-1])
        push(flat[0][1], j + 1)
        pops(flat[-1][0], j)
        for i, (s, k, rows) in enumerate(flat[:-1]):
            acc_pass(s, k, rows)
            push(flat[i + 1][1], j + 1)
            if flat[i + 1][0] != s:
                pops(s, j + 1)
        return carry

    lax.fori_loop(-1, n_tiles - 1, body, 0)
    top(n_tiles - 1)
    acc_pass(*flat[-1])
    pops(flat[-1][0], n_tiles - 1)


def when(cond, fn):
    if isinstance(cond, bool):
        if cond:
            fn()
    else:
        pl.when(cond)(fn)


def cols(j):
    return pl.ds(j * TN, TN) if isinstance(j, int) else pl.ds(pl.multiple_of(j * TN, TN), TN)


def wide(j):
    return pl.ds(pl.multiple_of(j * WIDE, WIDE), WIDE)


def gather_kernel(l_ref, b_ref, lg_ref, x1_ref, x2_ref, pf_ref, la, lb, lc, bbuf, pbuf, pin, obuf, own_sem, dsend, drecv, xsend, xrecv,
                  ysend, yrecv, fsend, frecv, bsem, psem, osem, gsem):
    me = lax.axis_index("col")
    core = lax.rem(me, 2)
    chip = me // 2
    sib = me + 1 - 2 * core
    oth = lax.rem(me + 2, 4)
    sib_oth = lax.rem(sib + 2, 4)
    strips = {4: la, 3: lb, 2: lc}

    def own_src(s, t):
        return l_ref.at[pl.ds(SUP * s, SUP), pl.ds(BLK * t, BLK)]

    def place(s, t, dev, far):
        if s not in strips:
            return lg_ref.at[LG_BASE[s] + 4 * t + dev]
        if t == s:
            slot = 4 * s + dev
        else:
            slot = (2 * s if far else 0) + 2 * t + lax.rem(dev, 2)
        return strips[s].at[:, pl.ds(pl.multiple_of(slot * BLK, BLK), BLK)]

    def own_copy(s, t):
        return pltpu.make_async_copy(own_src(s, t), place(s, t, me, False), own_sem.at[CHUNK_ID[s, t]])

    def remote(src, dst, send, recv, dev):
        return pltpu.make_async_remote_copy(src_ref=src, dst_ref=dst, send_sem=send, recv_sem=recv, device_id={"col": dev},
                                            device_id_type=pl.DeviceIdType.MESH)

    def to_sib(s, t):
        i = CHUNK_ID[s, t]
        return remote(own_src(s, t), place(s, t, me, False), dsend.at[i], drecv.at[i], sib)

    def cross(s, t, dev, do):
        i = CHUNK_ID[s, t]
        if t < s:
            do(remote(own_src(s, t), place(s, t, dev, True), xsend.at[i], xrecv.at[i], oth))
            return
        for r in ROWS:

            @pl.when(r >= dev)
            def _():
                src = l_ref.at[pl.ds(SUP * s + BLK * r, BLK), pl.ds(BLK * t, BLK)]
                dst = place(s, t, dev, True).at[pl.ds(BLK * r, BLK)]
                do(remote(src, dst, ysend.at[s, r], yrecv.at[s, r], oth))

    def forward(s, t):
        i = CHUNK_ID[s, t]
        here = place(s, t, oth, True)
        return remote(here, here, fsend.at[i], frecv.at[i], sib)

    def from_sib(s, t):
        i = CHUNK_ID[s, t]
        here = place(s, t, sib, False)
        return remote(here, here, dsend.at[i], drecv.at[i], sib)

    def from_fwd(s, t):
        i = CHUNK_ID[s, t]
        here = place(s, t, sib_oth, True)
        return remote(here, here, fsend.at[i], frecv.at[i], sib)

    def pass_on(s, t):
        cross(s, t, oth, lambda c: c.wait_recv())
        forward(s, t).start()

    jobs = [((3, 4), "part", NT), ((4,), "rest", NT), ((3,), "rest", NT), ((2,), "all", NT2)]
    cycles = {"part": lambda s: 2 * s * 512, "rest": lambda s: 2 * s * 512 + 1280, "all": lambda s: 4 * s * 512 + 1280}
    events, forced = [[] for _ in jobs], [[] for _ in jobs]
    clock, due, todo = 5.0, 4.0, []
    for s, t in CHUNKS:
        due += 11.3 if t < s else 9.9
        todo.append((due, (s, t)))
    for q, (sups, kind, n) in enumerate(jobs):
        while kind != "part" and todo and todo[0][1][0] >= sups[0]:
            clock = max(clock, todo[0][0])
            forced[q].append(todo.pop(0)[1])
        for j in range(n):
            while todo and clock > todo[0][0] + 1.5:
                events[q].append((j, todo.pop(0)[1]))
            clock += 2 * sum(map(cycles[kind], sups)) / 1850.0
    left = [st for _, st in todo]

    def b_copies(q, j, slot):
        s, kind = jobs[q][0][-1], jobs[q][1]
        dst = bbuf.at[slot]
        if kind == "part":
            return [pltpu.make_async_copy(b_ref.at[0:s, chip, :, wide(j)], dst.at[0:s], bsem.at[slot, 0])]
        far = pltpu.make_async_copy(b_ref.at[0:s, 1 - chip, :, wide(j)], dst.at[0:s], bsem.at[slot, 0])
        if kind == "rest":
            return [far, pltpu.make_async_copy(b_ref.at[s, :, :, wide(j)], dst.at[pl.ds(s, 2)], bsem.at[slot, 1])]
        return [
            pltpu.make_async_copy(b_ref.at[0:s, chip, :, wide(j)], dst.at[0:s], bsem.at[slot, 0]),
            pltpu.make_async_copy(b_ref.at[0:s, 1 - chip, :, wide(j)], dst.at[pl.ds(s, s)], bsem.at[slot, 2]),
            pltpu.make_async_copy(b_ref.at[s, :, :, wide(j)], dst.at[pl.ds(2 * s, 2)], bsem.at[slot, 1]),
        ]

    def run_job(q):
        sups, kind, n = jobs[q]
        nxt = q + 1 if q + 1 < len(jobs) else None

        def start_b(qq, j, slot):
            for c in b_copies(qq, j, slot):
                c.start()

        def x_copy(qq, j):
            (ss, *_), kk, _ = jobs[qq]
            dst = x1_ref.at[pl.ds(SUP * (ss - 3), SUP), wide(j)] if kk == "rest" else x2_ref.at[:, wide(j)]
            return pltpu.make_async_copy(obuf.at[j & 1], dst, osem.at[j & 1])

        def pf_out(i, j):
            return pltpu.make_async_copy(pbuf.at[i], pf_ref.at[i, :, wide(j)], gsem.at[i])

        def part_copy(qq, j):
            return pltpu.make_async_copy(pf_ref.at[jobs[qq][0][0] - 3, :, wide(j)], pin.at[j & 1], psem.at[j & 1])

        def body(j, carry):
            slot = j & 1

            @pl.when(j < n - 1)
            def _():
                start_b(q, j + 1, 1 - slot)
                if kind == "rest":
                    part_copy(q, j + 1).start()

            if nxt is not None:

                @pl.when(j == n - 1)
                def _():
                    start_b(nxt, 0, 0)
                    if jobs[nxt][1] == "rest":
                        part_copy(nxt, 0).start()

            if events[q]:
                hit = functools.reduce(jnp.logical_or, [j == jj for jj, _ in events[q]])

                @pl.when(hit)
                def _():
                    for jj, st in events[q]:
                        pl.when(j == jj)(functools.partial(pass_on, *st))

            if kind == "part":
                pl.when(j >= 1)(lambda: pf_out(1, j - 1).start())
            else:

                @pl.when(j == 0)
                def _():
                    if q == 1:
                        pf_out(1, NT - 1).start()
                        pf_out(0, NT - 1).wait()
                    else:
                        x_copy(q - 1, jobs[q - 1][2] - 1).start()
                        x_copy(q - 1, jobs[q - 1][2] - 2).wait()

                @pl.when(j == 1)
                def _():
                    x_copy(q, 0).start()
                    if q == 1:
                        pf_out(1, NT - 1).wait()
                    else:
                        x_copy(q - 1, jobs[q - 1][2] - 1).wait()

                @pl.when(j >= 2)
                def _():
                    x_copy(q, j - 1).start()
                    x_copy(q, j - 2).wait()

            if kind == "rest":
                part_copy(q, j).wait()
            for c in b_copies(q, j, slot):
                c.wait()
            for i, s in enumerate(sups):
                if kind == "part":
                    pl.when(j >= 1)(lambda: pf_out(i, j - 1).wait())
                    if i == 1:

                        @pl.when(j == 0)
                        def _():
                            for t in range(4):
                                own_copy(4, t).wait()
                                from_sib(4, t).wait_recv()

                base = 2 * s if kind == "rest" else 0
                for r in ROWS:
                    rows = slice(r * BLK, (r + 1) * BLK)
                    n_k = 2 * s if kind == "part" else 4 * s + r + 1 - base
                    for h in range(WIDE // DN):
                        half = slice(h * DN, (h + 1) * DN)
                        rhs = bbuf[slot, 0:(n_k + 1) // 2, :, half].reshape(-1, DN)[0:n_k * BLK]
                        v = jnp.dot(strips[s][rows, base * BLK:(base + n_k) * BLK], rhs, preferred_element_type=F32)
                        if kind == "part":
                            pbuf[i, rows, half] = v
                        elif kind == "rest":
                            obuf[slot, rows, half] = (v + pin[slot, rows, half]).astype(BF)
                        else:
                            obuf[slot, rows, half] = v.astype(BF)
                    if kind == "part" and (i, r) == (1, 0):
                        pf_out(0, j).start()
                    if kind == "all" and r == 2:

                        @pl.when(j == n - 1)
                        def _():
                            for st in left:
                                pass_on(*st)

            return carry

        lax.fori_loop(0, n, body, 0)
        if nxt is None:
            x_copy(q, n - 1).start()
            if n > 1:
                x_copy(q, n - 2).wait()
            else:
                x_copy(q - 1, jobs[q - 1][2] - 1).wait()
            x_copy(q, n - 1).wait()

    def inner():
        early = [(3, t) for t in range(3)] + [(4, t) for t in range(4)]
        for st in early[:3]:
            own_copy(*st).start()
        for c in b_copies(0, 0, 0):
            c.start()
        for st in early[3:]:
            own_copy(*st).start()
        barrier = pltpu.get_barrier_semaphore()
        for dev in (sib, oth):
            pl.semaphore_signal(barrier, inc=1, device_id={"col": dev}, device_id_type=pl.DeviceIdType.MESH)
        pl.semaphore_wait(barrier, 2)
        for st in early:
            to_sib(*st).start()
        for st in CHUNKS:
            cross(*st, me, lambda c: c.start())
        for st in CHUNKS:
            if st not in early:
                to_sib(*st).start()
                if st[0] >= 2:
                    own_copy(*st).start()

        for t in range(3):
            own_copy(3, t).wait()
            from_sib(3, t).wait_recv()
        run_job(0)
        for q, s in ((1, 4), (2, 3), (3, 2)):
            for st in forced[q]:
                pass_on(*st)
            for t in range(s + 1):
                if t == s or s == 2:
                    own_copy(s, t).wait()
                    from_sib(s, t).wait_recv()
                from_fwd(s, t).wait_recv()
            if s > 2:
                run_job(q)
        saves = []
        for k in range(12):
            t, u = k % 4 // 2, k % 2
            kb = k if k >= 8 else 4 * t + 2 * (chip if k < 4 else 1 - chip) + u
            saves.append(pltpu.make_async_copy(lc.at[:, pl.ds(k * BLK, BLK)], lg_ref.at[LG_BASE[2] + kb], gsem.at[2 + k]))
        for c in saves:
            c.start()
        run_job(3)
        for c in saves:
            c.wait()
        for s in (1, 0):
            for t in range(s + 1):
                from_sib(s, t).wait_recv()
                from_fwd(s, t).wait_recv()
        for s, t in CHUNKS:
            to_sib(s, t).wait_send()
            cross(s, t, me, lambda c: c.wait_send())
            forward(s, t).wait_send()

    inner()


def finish_kernel(l_ref, b_ref, lg_ref, x1_ref, x2_ref, x_ref, lbuf, bbuf, obuf, cbuf, dbuf, lsem, bsem, osem, csem, dsem):
    me = lax.axis_index("col")
    jobs = [(0, N0, (0, 1)), (N0, N1, (0, 1, 2))]

    def l_copies(s):
        base = LG_BASE[s]
        if s == 2:
            return [pltpu.make_async_copy(lg_ref.at[pl.ds(base, 12)], lbuf.at[pl.ds(base, 12)], lsem.at[base])]
        out = []
        for t in range(s + 1):
            for d in range(4):
                at = base + 4 * t + lax.rem(me + d, 4)
                src = l_ref.at[pl.ds(SUP * s, SUP), pl.ds(BLK * t, BLK)] if d == 0 else lg_ref.at[at]
                out.append(pltpu.make_async_copy(src, lbuf.at[at], lsem.at[base + 4 * t + d]))
        return out

    def b_copy(q, j, slot):
        n = 4 * len(jobs[q][2])
        return pltpu.make_async_copy(b_ref.at[0:n, :, cols(jobs[q][0] + j)], bbuf.at[slot, 0:n], bsem.at[slot])

    def run_job(q, accs):
        first, n, sups = jobs[q]
        nxt = q + 1 if q + 1 < len(jobs) else None
        lasts = len(sups) - 1

        def out_copy(u, j):
            slot = j & 1
            return pltpu.make_async_copy(obuf.at[slot, u], x_ref.at[pl.ds(SUP * sups[u], SUP), cols(first + j)], osem.at[slot, u])

        if q == 0:
            chunks = n
            rows = SUP // chunks

            def c_in(j):
                return pltpu.make_async_copy(x2_ref.at[pl.ds(pl.multiple_of(j * rows, rows), rows), :], dbuf.at[j & 1], dsem.at[0, j & 1])

            def c_out(j):
                return pltpu.make_async_copy(
                    dbuf.at[j & 1], x_ref.at[pl.ds(pl.multiple_of(2 * SUP + j * rows, rows), rows), pl.ds(0, N0 * TN)], dsem.at[1, j & 1])
        else:
            chunks = n
            rows = COPY

            def part(j):
                return pl.multiple_of(jnp.minimum(j * rows, 2 * SUP - rows), 16)

            def c_in(j):
                return pltpu.make_async_copy(x1_ref.at[pl.ds(part(j), rows), :], cbuf.at[j & 1], csem.at[0, j & 1])

            def c_out(j):
                return pltpu.make_async_copy(
                    cbuf.at[j & 1], x_ref.at[pl.ds(3 * SUP + part(j), rows), :], csem.at[1, j & 1])

        def top(j):
            last = isinstance(j, int)
            if not last:
                b_copy(q, j + 1, (j + 1) & 1).wait()
                lo = -1 if q == 0 else 0
                pl.when(jnp.logical_and(j >= lo, j < n - 2))(lambda: b_copy(q, j + 2, j & 1).start())
                if nxt is not None:
                    pl.when(j == n - 2)(lambda: b_copy(nxt, 0, 0).start())
            elif nxt is not None:
                b_copy(nxt, 1, 1).start()
            for u in range(len(sups)):
                if u < lasts:
                    when(True if last else j >= 0, lambda: out_copy(u, j).start())
                    when(True if last else j >= 1, lambda: out_copy(u, j - 1).wait())
                else:
                    when(True if last else j >= 1, lambda: out_copy(u, j - 1).start())
                    when(True if last else j >= 2, lambda: out_copy(u, j - 2).wait())
            if not last:
                pl.when(jnp.logical_and(j >= 1, j <= chunks))(lambda: c_out(j - 1).wait())
                pl.when(j + 1 < chunks)(lambda: c_in(j + 1).start())
            if not last or j < chunks:

                def move():
                    c_in(j).wait()
                    c_out(j).start()

                when(True if last else jnp.logical_and(j >= 0, j < chunks), move)

        def lhs_of(u, k, r):
            return lbuf[LG_BASE[sups[u]] + k, r * BLK:(r + 1) * BLK, :]

        def rhs_of(k, m, j):
            return bbuf[j & 1, k, :, m * BLK:(m + 1) * BLK]

        def emit(u, j, r, m, v):
            obuf[j & 1, u, r * BLK:(r + 1) * BLK, m * BLK:(m + 1) * BLK] = v.astype(BF)

        subs = [diag_passes(4 * s) + [(4 * s, ROWS)] + [(k, ROWS) for k in range(4 * s)] for s in sups]
        run_tiles(accs, subs, lhs_of, rhs_of, emit, top, n)
        out_copy(lasts, n - 1).start()
        if chunks == n:
            c_out(n - 2).wait()
            c_out(n - 1).wait()
        for u in range(len(sups)):
            if u == lasts:
                out_copy(u, n - 2).wait()
            out_copy(u, n - 1).wait()

    def inner(*refs):
        accs = (refs[:4], refs[4:])
        b_copy(0, 0, 0).start()
        for s in (0, 1):
            for c in l_copies(s):
                c.start()
        for s in (0, 1):
            for c in l_copies(s):
                c.wait()
        for c in l_copies(2):
            c.start()
        run_job(0, accs)
        for c in l_copies(2):
            c.wait()
        run_job(1, accs)

    pl.run_scoped(inner, *[pltpu.ACC(m)((BLK, BLK), F32) for m in range(2) for _ in ROWS])


def solution(mesh):
    hbm = pl.BlockSpec(memory_space=pltpu.HBM)
    dma = pltpu.SemaphoreType.DMA

    def local_product(l_cols, b_cols):
        order, width = b_cols.shape
        b4 = b_cols.reshape(NSUP, 2, 2 * BLK, width)
        b3 = b_cols.reshape(4 * NSUP, BLK, width)
        lg, x1, x2, _ = pl.pallas_call(
            gather_kernel,
            out_shape=(
                jax.ShapeDtypeStruct((24, SUP, BLK), BF),
                jax.ShapeDtypeStruct((2 * SUP, width), BF),
                jax.ShapeDtypeStruct((SUP, N0 * TN), BF),
                jax.ShapeDtypeStruct((2, SUP, width), F32),
            ),
            in_specs=[hbm] * 2,
            out_specs=(hbm,) * 4,
            scratch_shapes=[
                pltpu.VMEM((SUP, 20 * BLK), BF),
                pltpu.VMEM((SUP, 16 * BLK), BF),
                pltpu.VMEM((SUP, 12 * BLK), BF),
                pltpu.VMEM((2, 6, 2 * BLK, WIDE), BF),
                pltpu.VMEM((2, SUP, WIDE), F32),
                pltpu.VMEM((2, SUP, WIDE), F32),
                pltpu.VMEM((2, SUP, WIDE), BF),
            ] + [dma((15,))] * 5 + [dma((5, 4))] * 2 + [dma((15,))] * 2 + [dma((2, 3)), dma((2,)), dma((2,)), dma((14,))],
            compiler_params=pltpu.CompilerParams(vmem_limit_bytes=62 * 1024 * 1024, collective_id=0, has_side_effects=True),
        )(l_cols, b4)
        return pl.pallas_call(
            finish_kernel,
            out_shape=jax.ShapeDtypeStruct((order, width), BF),
            in_specs=[hbm] * 5,
            out_specs=hbm,
            scratch_shapes=[
                pltpu.VMEM((24, SUP, BLK), BF),
                pltpu.VMEM((2, 12, BLK, TN), BF),
                pltpu.VMEM((2, 3, SUP, TN), BF),
                pltpu.VMEM((2, COPY, width), BF),
                pltpu.VMEM((2, SUP // N0, N0 * TN), BF),
            ] + [dma((24,)), dma((2,)), dma((2, 3)), dma((2, 2)), dma((2, 2))],
            compiler_params=pltpu.CompilerParams(vmem_limit_bytes=62 * 1024 * 1024),
        )(l_cols, b3, lg, x1, x2)

    return jax.shard_map(local_product, mesh=mesh, in_specs=(P("batch", "col"), P("batch", "col")), out_specs=P("batch", "col"), check_vma=False)
```

```python
import functools

import jax
import jax.numpy as jnp
from jax import lax
from jax.experimental import pallas as pl
from jax.experimental.pallas import tpu as pltpu
from jax.sharding import PartitionSpec as P

BF = jnp.bfloat16
F32 = jnp.float32
BLK = 256
SUP = 4 * BLK
TN = 512
NSUP = 5
WIDE = 1024
DN = 512
NT = 8
NT2 = 2
N0 = NT2 * WIDE // TN
N1 = (NT - NT2) * WIDE // TN
COPY = -(-2 * SUP // N1 // 16) * 16
ROWS = (0, 1, 2, 3)

CHUNKS = [(s, t) for s in (4, 3, 2, 1, 0) for t in range(s + 1)]
CHUNK_ID = {st: i for i, st in enumerate(CHUNKS)}
LG_BASE = {0: 0, 1: 4, 2: 12}


def diag_passes(base):
    return [(base + 1, (1, 2, 3)), (base + 2, (2, 3)), (base + 3, (3,))]


def run_tiles(accs, subs, lhs_of, rhs_of, emit, top, n_tiles):
    flat = [(s, k, rows) for s, passes in enumerate(subs) for k, rows in passes]

    def push(k, j):
        for m in range(2):
            pltpu.matmul_push_rhs(rhs_of(k, m, j), staging_register=0, mxu_index=m)

    def acc_pass(s, k, rows):
        for i, r in enumerate(rows):
            lhs = lhs_of(s, k, r)
            for m in range(2):
                pltpu.matmul_acc_lhs(accs[m][r], lhs, load_staged_rhs=0 if i == 0 else None)

    def pops(s, j):
        for r in ROWS:
            for m in range(2):
                emit(s, j, r, m, pltpu.matmul_pop(accs[m][r]))

    def body(j, carry):
        top(j)
        acc_pass(*flat[-1])
        push(flat[0][1], j + 1)
        pops(flat[-1][0], j)
        for i, (s, k, rows) in enumerate(flat[:-1]):
            acc_pass(s, k, rows)
            push(flat[i + 1][1], j + 1)
            if flat[i + 1][0] != s:
                pops(s, j + 1)
        return carry

    lax.fori_loop(-1, n_tiles - 1, body, 0)
    top(n_tiles - 1)
    acc_pass(*flat[-1])
    pops(flat[-1][0], n_tiles - 1)


def when(cond, fn):
    if isinstance(cond, bool):
        if cond:
            fn()
    else:
        pl.when(cond)(fn)


def cols(j):
    return pl.ds(j * TN, TN) if isinstance(j, int) else pl.ds(pl.multiple_of(j * TN, TN), TN)


def wide(j):
    return pl.ds(pl.multiple_of(j * WIDE, WIDE), WIDE)


def gather_kernel(l_ref, b_ref, lg_ref, x1_ref, x2_ref, pf_ref, la, lb, lc, bbuf, pbuf, pin, obuf, own_sem, dsend, drecv, xsend, xrecv,
                  ysend, yrecv, fsend, frecv, bsem, psem, osem, gsem):
    me = lax.axis_index("col")
    core = lax.rem(me, 2)
    chip = me // 2
    sib = me + 1 - 2 * core
    oth = lax.rem(me + 2, 4)
    sib_oth = lax.rem(sib + 2, 4)
    strips = {4: la, 3: lb, 2: lc}

    def own_src(s, t):
        return l_ref.at[pl.ds(SUP * s, SUP), pl.ds(BLK * t, BLK)]

    def place(s, t, dev, far):
        if s not in strips:
            return lg_ref.at[LG_BASE[s] + 4 * t + dev]
        if t == s:
            slot = 4 * s + dev
        else:
            slot = (2 * s if far else 0) + 2 * t + lax.rem(dev, 2)
        return strips[s].at[:, pl.ds(pl.multiple_of(slot * BLK, BLK), BLK)]

    def own_copy(s, t):
        return pltpu.make_async_copy(own_src(s, t), place(s, t, me, False), own_sem.at[CHUNK_ID[s, t]])

    def remote(src, dst, send, recv, dev):
        return pltpu.make_async_remote_copy(src_ref=src, dst_ref=dst, send_sem=send, recv_sem=recv, device_id={"col": dev},
                                            device_id_type=pl.DeviceIdType.MESH)

    def to_sib(s, t):
        i = CHUNK_ID[s, t]
        return remote(own_src(s, t), place(s, t, me, False), dsend.at[i], drecv.at[i], sib)

    def cross(s, t, dev, do):
        i = CHUNK_ID[s, t]
        if t < s:
            do(remote(own_src(s, t), place(s, t, dev, True), xsend.at[i], xrecv.at[i], oth))
            return
        for r in ROWS:

            @pl.when(r >= dev)
            def _():
                src = l_ref.at[pl.ds(SUP * s + BLK * r, BLK), pl.ds(BLK * t, BLK)]
                dst = place(s, t, dev, True).at[pl.ds(BLK * r, BLK)]
                do(remote(src, dst, ysend.at[s, r], yrecv.at[s, r], oth))

    def forward(s, t):
        i = CHUNK_ID[s, t]
        here = place(s, t, oth, True)
        return remote(here, here, fsend.at[i], frecv.at[i], sib)

    def from_sib(s, t):
        i = CHUNK_ID[s, t]
        here = place(s, t, sib, False)
        return remote(here, here, dsend.at[i], drecv.at[i], sib)

    def from_fwd(s, t):
        i = CHUNK_ID[s, t]
        here = place(s, t, sib_oth, True)
        return remote(here, here, fsend.at[i], frecv.at[i], sib)

    def pass_on(s, t):
        cross(s, t, oth, lambda c: c.wait_recv())
        forward(s, t).start()

    jobs = [((3, 4), "part", NT), ((4,), "rest", NT), ((3,), "rest", NT), ((2,), "all", NT2)]
    cycles = {"part": lambda s: 2 * s * 512, "rest": lambda s: 2 * s * 512 + 1280, "all": lambda s: 4 * s * 512 + 1280}
    events, forced = [[] for _ in jobs], [[] for _ in jobs]
    clock, due, todo = 5.0, 3.5, []
    for s, t in CHUNKS:
        due += 11.3 if t < s else 9.9
        todo.append((due, (s, t)))
    for q, (sups, kind, n) in enumerate(jobs):
        while kind != "part" and todo and todo[0][1][0] >= sups[0]:
            clock = max(clock, todo[0][0])
            forced[q].append(todo.pop(0)[1])
        for j in range(n):
            while todo and clock > todo[0][0] + 0.3:
                events[q].append((j, todo.pop(0)[1]))
            clock += 2 * sum(map(cycles[kind], sups)) / 1850.0
    left = [st for _, st in todo]

    def b_copies(q, j, slot):
        s, kind = jobs[q][0][-1], jobs[q][1]
        dst = bbuf.at[slot]
        if kind == "part":
            return [pltpu.make_async_copy(b_ref.at[0:s, chip, :, wide(j)], dst.at[0:s], bsem.at[slot, 0])]
        far = pltpu.make_async_copy(b_ref.at[0:s, 1 - chip, :, wide(j)], dst.at[0:s], bsem.at[slot, 0])
        if kind == "rest":
            return [far, pltpu.make_async_copy(b_ref.at[s, :, :, wide(j)], dst.at[pl.ds(s, 2)], bsem.at[slot, 1])]
        return [
            pltpu.make_async_copy(b_ref.at[0:s, chip, :, wide(j)], dst.at[0:s], bsem.at[slot, 0]),
            pltpu.make_async_copy(b_ref.at[0:s, 1 - chip, :, wide(j)], dst.at[pl.ds(s, s)], bsem.at[slot, 2]),
            pltpu.make_async_copy(b_ref.at[s, :, :, wide(j)], dst.at[pl.ds(2 * s, 2)], bsem.at[slot, 1]),
        ]

    def run_job(q):
        sups, kind, n = jobs[q]
        nxt = q + 1 if q + 1 < len(jobs) else None

        def start_b(qq, j, slot):
            for c in b_copies(qq, j, slot):
                c.start()

        def x_copy(qq, j):
            (ss, *_), kk, _ = jobs[qq]
            dst = x1_ref.at[pl.ds(SUP * (ss - 3), SUP), wide(j)] if kk == "rest" else x2_ref.at[:, wide(j)]
            return pltpu.make_async_copy(obuf.at[j & 1], dst, osem.at[j & 1])

        def pf_out(i, j):
            return pltpu.make_async_copy(pbuf.at[i], pf_ref.at[i, :, wide(j)], gsem.at[i])

        def part_copy(qq, j):
            return pltpu.make_async_copy(pf_ref.at[jobs[qq][0][0] - 3, :, wide(j)], pin.at[j & 1], psem.at[j & 1])

        def body(j, carry):
            slot = j & 1

            @pl.when(j < n - 1)
            def _():
                start_b(q, j + 1, 1 - slot)
                if kind == "rest":
                    part_copy(q, j + 1).start()

            if nxt is not None:

                @pl.when(j == n - 1)
                def _():
                    start_b(nxt, 0, 0)
                    if jobs[nxt][1] == "rest":
                        part_copy(nxt, 0).start()

            if events[q]:
                hit = functools.reduce(jnp.logical_or, [j == jj for jj, _ in events[q]])

                @pl.when(hit)
                def _():
                    for jj, st in events[q]:
                        pl.when(j == jj)(functools.partial(pass_on, *st))

            if kind == "part":
                pl.when(j >= 1)(lambda: pf_out(1, j - 1).start())
            else:

                @pl.when(j == 0)
                def _():
                    if q == 1:
                        pf_out(1, NT - 1).start()
                        pf_out(0, NT - 1).wait()
                    else:
                        x_copy(q - 1, jobs[q - 1][2] - 1).start()
                        x_copy(q - 1, jobs[q - 1][2] - 2).wait()

                @pl.when(j == 1)
                def _():
                    x_copy(q, 0).start()
                    if q == 1:
                        pf_out(1, NT - 1).wait()
                    else:
                        x_copy(q - 1, jobs[q - 1][2] - 1).wait()

                @pl.when(j >= 2)
                def _():
                    x_copy(q, j - 1).start()
                    x_copy(q, j - 2).wait()

            if kind == "rest":
                part_copy(q, j).wait()
            for c in b_copies(q, j, slot):
                c.wait()
            for i, s in enumerate(sups):
                if kind == "part":
                    pl.when(j >= 1)(lambda: pf_out(i, j - 1).wait())
                    if i == 1:

                        @pl.when(j == 0)
                        def _():
                            for t in range(4):
                                own_copy(4, t).wait()
                                from_sib(4, t).wait_recv()

                base = 2 * s if kind == "rest" else 0
                for r in ROWS:
                    rows = slice(r * BLK, (r + 1) * BLK)
                    n_k = 2 * s if kind == "part" else 4 * s + r + 1 - base
                    for h in range(WIDE // DN):
                        half = slice(h * DN, (h + 1) * DN)
                        rhs = bbuf[slot, 0:(n_k + 1) // 2, :, half].reshape(-1, DN)[0:n_k * BLK]
                        v = jnp.dot(strips[s][rows, base * BLK:(base + n_k) * BLK], rhs, preferred_element_type=F32)
                        if kind == "part":
                            pbuf[i, rows, half] = v
                        elif kind == "rest":
                            obuf[slot, rows, half] = (v + pin[slot, rows, half]).astype(BF)
                        else:
                            obuf[slot, rows, half] = v.astype(BF)
                    if kind == "part" and (i, r) == (1, 0):
                        pf_out(0, j).start()
                    if kind == "all" and r == 2:

                        @pl.when(j == n - 1)
                        def _():
                            for st in left:
                                pass_on(*st)

            return carry

        lax.fori_loop(0, n, body, 0)
        if nxt is None:
            x_copy(q, n - 1).start()
            if n > 1:
                x_copy(q, n - 2).wait()
            else:
                x_copy(q - 1, jobs[q - 1][2] - 1).wait()
            x_copy(q, n - 1).wait()

    def inner():
        early = [(3, t) for t in range(3)] + [(4, t) for t in range(4)]
        for st in early[:3]:
            own_copy(*st).start()
        for c in b_copies(0, 0, 0):
            c.start()
        for st in early[3:]:
            own_copy(*st).start()
        barrier = pltpu.get_barrier_semaphore()
        for dev in (sib, oth):
            pl.semaphore_signal(barrier, inc=1, device_id={"col": dev}, device_id_type=pl.DeviceIdType.MESH)
        pl.semaphore_wait(barrier, 2)
        for st in early:
            to_sib(*st).start()
        for st in CHUNKS:
            cross(*st, me, lambda c: c.start())
        for st in CHUNKS:
            if st not in early:
                to_sib(*st).start()
                if st[0] >= 2:
                    own_copy(*st).start()

        for t in range(3):
            own_copy(3, t).wait()
            from_sib(3, t).wait_recv()
        run_job(0)
        for q, s in ((1, 4), (2, 3), (3, 2)):
            for st in forced[q]:
                pass_on(*st)
            for t in range(s + 1):
                if t == s or s == 2:
                    own_copy(s, t).wait()
                    from_sib(s, t).wait_recv()
                from_fwd(s, t).wait_recv()
            if s > 2:
                run_job(q)
        saves = []
        for k in range(12):
            t, u = k % 4 // 2, k % 2
            kb = k if k >= 8 else 4 * t + 2 * (chip if k < 4 else 1 - chip) + u
            saves.append(pltpu.make_async_copy(lc.at[:, pl.ds(k * BLK, BLK)], lg_ref.at[LG_BASE[2] + kb], gsem.at[2 + k]))
        for c in saves:
            c.start()
        run_job(3)
        for c in saves:
            c.wait()
        for s in (1, 0):
            for t in range(s + 1):
                from_sib(s, t).wait_recv()
                from_fwd(s, t).wait_recv()
        for s, t in CHUNKS:
            to_sib(s, t).wait_send()
            cross(s, t, me, lambda c: c.wait_send())
            forward(s, t).wait_send()

    inner()


def finish_kernel(l_ref, b_ref, lg_ref, x1_ref, x2_ref, x_ref, lbuf, bbuf, obuf, cbuf, dbuf, lsem, bsem, osem, csem, dsem):
    me = lax.axis_index("col")
    jobs = [(0, N0, (0, 1)), (N0, N1, (0, 1, 2))]

    def l_copies(s):
        base = LG_BASE[s]
        if s == 2:
            return [pltpu.make_async_copy(lg_ref.at[pl.ds(base, 12)], lbuf.at[pl.ds(base, 12)], lsem.at[base])]
        out = []
        for t in range(s + 1):
            for d in range(4):
                at = base + 4 * t + lax.rem(me + d, 4)
                src = l_ref.at[pl.ds(SUP * s, SUP), pl.ds(BLK * t, BLK)] if d == 0 else lg_ref.at[at]
                out.append(pltpu.make_async_copy(src, lbuf.at[at], lsem.at[base + 4 * t + d]))
        return out

    def b_copy(q, j, slot):
        n = 4 * len(jobs[q][2])
        return pltpu.make_async_copy(b_ref.at[0:n, :, cols(jobs[q][0] + j)], bbuf.at[slot, 0:n], bsem.at[slot])

    def run_job(q, accs):
        first, n, sups = jobs[q]
        nxt = q + 1 if q + 1 < len(jobs) else None
        lasts = len(sups) - 1

        def out_copy(u, j):
            slot = j & 1
            return pltpu.make_async_copy(obuf.at[slot, u], x_ref.at[pl.ds(SUP * sups[u], SUP), cols(first + j)], osem.at[slot, u])

        if q == 0:
            chunks = n
            rows = SUP // chunks

            def c_in(j):
                return pltpu.make_async_copy(x2_ref.at[pl.ds(pl.multiple_of(j * rows, rows), rows), :], dbuf.at[j & 1], dsem.at[0, j & 1])

            def c_out(j):
                return pltpu.make_async_copy(
                    dbuf.at[j & 1], x_ref.at[pl.ds(pl.multiple_of(2 * SUP + j * rows, rows), rows), pl.ds(0, N0 * TN)], dsem.at[1, j & 1])
        else:
            chunks = n
            rows = COPY

            def part(j):
                return pl.multiple_of(jnp.minimum(j * rows, 2 * SUP - rows), 16)

            def c_in(j):
                return pltpu.make_async_copy(x1_ref.at[pl.ds(part(j), rows), :], cbuf.at[j & 1], csem.at[0, j & 1])

            def c_out(j):
                return pltpu.make_async_copy(
                    cbuf.at[j & 1], x_ref.at[pl.ds(3 * SUP + part(j), rows), :], csem.at[1, j & 1])

        def top(j):
            last = isinstance(j, int)
            if not last:
                b_copy(q, j + 1, (j + 1) & 1).wait()
                lo = -1 if q == 0 else 0
                pl.when(jnp.logical_and(j >= lo, j < n - 2))(lambda: b_copy(q, j + 2, j & 1).start())
                if nxt is not None:
                    pl.when(j == n - 2)(lambda: b_copy(nxt, 0, 0).start())
            elif nxt is not None:
                b_copy(nxt, 1, 1).start()
            for u in range(len(sups)):
                if u < lasts:
                    when(True if last else j >= 0, lambda: out_copy(u, j).start())
                    when(True if last else j >= 1, lambda: out_copy(u, j - 1).wait())
                else:
                    when(True if last else j >= 1, lambda: out_copy(u, j - 1).start())
                    when(True if last else j >= 2, lambda: out_copy(u, j - 2).wait())
            if not last:
                pl.when(jnp.logical_and(j >= 1, j <= chunks))(lambda: c_out(j - 1).wait())
                pl.when(j + 1 < chunks)(lambda: c_in(j + 1).start())
            if not last or j < chunks:

                def move():
                    c_in(j).wait()
                    c_out(j).start()

                when(True if last else jnp.logical_and(j >= 0, j < chunks), move)

        def lhs_of(u, k, r):
            return lbuf[LG_BASE[sups[u]] + k, r * BLK:(r + 1) * BLK, :]

        def rhs_of(k, m, j):
            return bbuf[j & 1, k, :, m * BLK:(m + 1) * BLK]

        def emit(u, j, r, m, v):
            obuf[j & 1, u, r * BLK:(r + 1) * BLK, m * BLK:(m + 1) * BLK] = v.astype(BF)

        subs = [diag_passes(4 * s) + [(4 * s, ROWS)] + [(k, ROWS) for k in range(4 * s)] for s in sups]
        run_tiles(accs, subs, lhs_of, rhs_of, emit, top, n)
        out_copy(lasts, n - 1).start()
        if chunks == n:
            c_out(n - 2).wait()
            c_out(n - 1).wait()
        for u in range(len(sups)):
            if u == lasts:
                out_copy(u, n - 2).wait()
            out_copy(u, n - 1).wait()

    def inner(*refs):
        accs = (refs[:4], refs[4:])
        b_copy(0, 0, 0).start()
        for s in (0, 1):
            for c in l_copies(s):
                c.start()
        for s in (0, 1):
            for c in l_copies(s):
                c.wait()
        for c in l_copies(2):
            c.start()
        run_job(0, accs)
        for c in l_copies(2):
            c.wait()
        run_job(1, accs)

    pl.run_scoped(inner, *[pltpu.ACC(m)((BLK, BLK), F32) for m in range(2) for _ in ROWS])


def solution(mesh):
    hbm = pl.BlockSpec(memory_space=pltpu.HBM)
    dma = pltpu.SemaphoreType.DMA

    def local_product(l_cols, b_cols):
        order, width = b_cols.shape
        b4 = b_cols.reshape(NSUP, 2, 2 * BLK, width)
        b3 = b_cols.reshape(4 * NSUP, BLK, width)
        lg, x1, x2, _ = pl.pallas_call(
            gather_kernel,
            out_shape=(
                jax.ShapeDtypeStruct((24, SUP, BLK), BF),
                jax.ShapeDtypeStruct((2 * SUP, width), BF),
                jax.ShapeDtypeStruct((SUP, N0 * TN), BF),
                jax.ShapeDtypeStruct((2, SUP, width), F32),
            ),
            in_specs=[hbm] * 2,
            out_specs=(hbm,) * 4,
            scratch_shapes=[
                pltpu.VMEM((SUP, 20 * BLK), BF),
                pltpu.VMEM((SUP, 16 * BLK), BF),
                pltpu.VMEM((SUP, 12 * BLK), BF),
                pltpu.VMEM((2, 6, 2 * BLK, WIDE), BF),
                pltpu.VMEM((2, SUP, WIDE), F32),
                pltpu.VMEM((2, SUP, WIDE), F32),
                pltpu.VMEM((2, SUP, WIDE), BF),
            ] + [dma((15,))] * 5 + [dma((5, 4))] * 2 + [dma((15,))] * 2 + [dma((2, 3)), dma((2,)), dma((2,)), dma((14,))],
            compiler_params=pltpu.CompilerParams(vmem_limit_bytes=62 * 1024 * 1024, collective_id=0, has_side_effects=True),
        )(l_cols, b4)
        return pl.pallas_call(
            finish_kernel,
            out_shape=jax.ShapeDtypeStruct((order, width), BF),
            in_specs=[hbm] * 5,
            out_specs=hbm,
            scratch_shapes=[
                pltpu.VMEM((24, SUP, BLK), BF),
                pltpu.VMEM((2, 12, BLK, TN), BF),
                pltpu.VMEM((2, 3, SUP, TN), BF),
                pltpu.VMEM((2, COPY, width), BF),
                pltpu.VMEM((2, SUP // N0, N0 * TN), BF),
            ] + [dma((24,)), dma((2,)), dma((2, 3)), dma((2, 2)), dma((2, 2))],
            compiler_params=pltpu.CompilerParams(vmem_limit_bytes=62 * 1024 * 1024),
        )(l_cols, b3, lg, x1, x2)

    return jax.shard_map(local_product, mesh=mesh, in_specs=(P("batch", "col"), P("batch", "col")), out_specs=P("batch", "col"), check_vma=False)
```
